32 devices in a mesh: row: 4 (over z), col: 8 (over y, x, core).
Axes of the slice: x: 2, y: 2, z: 4, core: 2. Of those that a mesh axis runs over, the one named last changes fastest.
Arguments:
- factor: bfloat16 [32768, 5, 1024], P('col', None, 'row'), may hold values from -0.0625 to 0.0625
- diag_inverse: bfloat16 [5, 1024, 1024], P(None, 'row'), may hold values from -1 to 2
- right_side: float32 [16, 32, 1024], P(None, 'col', 'row'), may hold values from -6 to 6
- tile_order: int32 [32], replicated, may hold values from 0 to 31, each once
- live_segments: int32 [16], replicated, may hold values from 2 to 5
Outputs:
- result: float32 [16, 32, 1024], P(None, 'col', 'row')
The draws below stay inside these ranges and needn't reach their ends.
Inputs may be any that keep to these rules, and one draw needn't show every extreme that they name: `tile_order`: each of 0 to 31 appears once.
All inputs are finite; a program needn't handle non-finite values.
Results may differ from the reference program's by a relative error of at most 0.0019.
Values may be sent and summed in bfloat16 or wider, within the bound.
A program may use at most 64 MiB of HBM per device.

```python
import math
import jax
import jax.numpy as jnp
from jax import lax

TB = 1024
NRHS = 16
SECTIONS = 5
K = 32
N = 32768


def draw_diag_inverse(key, part):
    identity = jnp.broadcast_to(jnp.eye(TB, dtype=jnp.float32), (SECTIONS, TB, TB))
    noise = jax.random.normal(key, (SECTIONS, TB, TB), jnp.float32) * (0.4 / math.sqrt(TB))
    return (identity + noise).astype(jnp.bfloat16)


def place_ends(values, stream_key, low, top_value):
    shape = values.shape
    place = [jax.random.randint(jax.random.fold_in(stream_key, axis), (), 0, shape[axis]) for axis in range(len(shape))]
    values = values.at[tuple(place)].set(low)
    longest = shape.index(max(shape))
    place[longest] = (place[longest] + 1) % shape[longest]
    return values.at[tuple(place)].set(top_value)


def level_of(own_key, shape, cuts, least, high):
    gain = 1.0
    for position, blocks in cuts:
        heights = jax.random.uniform(jax.random.fold_in(jax.random.fold_in(own_key, 6), position), (blocks,), jnp.float32, least / len(cuts), high / len(cuts))
        gain = gain * jnp.repeat(jnp.exp(heights), shape[position] // blocks).reshape((-1,) + (1,) * (len(shape) - 1 - position))
    return gain


def scatter_about(rng, extent, scale, limit, cuts=(), kind=jnp.bfloat16):
    loudness = level_of(rng, extent, cuts, -0.22, 0.18) if cuts else 1.0
    entries = jax.random.normal(rng, extent, jnp.float32) * scale * loudness
    return jnp.minimum(jnp.maximum(entries, -limit), limit).astype(kind)


def setup_inputs(seed: int = 0) -> dict:
    key_of = jax.random.split(jax.random.key(seed), 6)
    factor = scatter_about(key_of[0], (N, SECTIONS, TB), (2 * SECTIONS * TB) ** -0.5, 0.0625, ((0, 8), (2, 4)))
    diag_inverse = draw_diag_inverse(jax.random.fold_in(key_of[5], 71), 0)
    right_side = scatter_about(key_of[2], (NRHS, K, TB), 1.0, 6.0, ((1, 8), (2, 4)), jnp.float32)
    tile_order = jax.random.permutation(key_of[3], K).astype(jnp.int32)
    live_segments = place_ends(jax.random.randint(key_of[4], (NRHS,), SECTIONS // 2, SECTIONS + 1), jax.random.fold_in(key_of[4], 1), SECTIONS // 2, SECTIONS).astype(jnp.int32)
    return dict(factor=factor, diag_inverse=diag_inverse, right_side=right_side, tile_order=tile_order, live_segments=live_segments)


def reference(factor, diag_inverse, right_side, tile_order, live_segments):
    segment_limit = live_segments.astype(jnp.int32)
    partial_value = jnp.zeros((NRHS, K * TB), jnp.float32)
    result = jnp.zeros((NRHS, K, TB), jnp.float32)
    for section in range(SECTIONS):
        slot_id = tile_order[section].astype(jnp.int32)
        offset = (slot_id * TB).astype(jnp.int32)
        rhs_tile = lax.dynamic_index_in_dim(right_side, slot_id, 1, keepdims=False)
        remaining = rhs_tile - lax.dynamic_slice_in_dim(partial_value, offset, TB, 1)
        inverse = diag_inverse[section].astype(jnp.float32)
        solved = lax.dot_general(remaining, inverse, (((1,), (1,)), ((), ())),
                                 precision=lax.Precision.HIGHEST, preferred_element_type=jnp.float32)
        is_live = (section < segment_limit)[:, None]
        sent_block = jnp.where(is_live, solved, jnp.zeros_like(solved)).astype(jnp.bfloat16)
        partial_value = partial_value + lax.dot_general(sent_block, factor[:, section, :], (((1,), (1,)), ((), ())),
                                            preferred_element_type=jnp.float32)
        stored = jnp.where(is_live, solved, remaining)
        result = lax.dynamic_update_slice_in_dim(result, stored[:, None, :], slot_id, 1)
    slot_ids = jnp.arange(K, dtype=jnp.int32)
    visited = jnp.any(slot_ids[:, None] == tile_order[:SECTIONS][None, :], axis=1)
    trailing = right_side - partial_value.reshape(NRHS, K, TB)
    return jnp.where(visited[None, :, None], result, trailing)
```

```python
import functools
import jax
import jax.numpy as jnp
from jax import lax
from jax.experimental import pallas as pl
from jax.experimental.pallas import tpu as pltpu
from jax.sharding import PartitionSpec as P

MESH = pl.DeviceIdType.MESH
NT = (((1,), (1,)), ((), ()))


def remote(src, dst, send_sem, recv_sem, axis, peer):
    return pltpu.make_async_remote_copy(
        src_ref=src, dst_ref=dst, send_sem=send_sem, recv_sem=recv_sem,
        device_id={axis: peer}, device_id_type=MESH,
    )


def kernel(
    rows, cols, factor_hbm, inverse_hbm, rhs, order, live, out,
    factor, inverse, first, part_out, part_in, sent_all, stored, acc, tail_out, tail_in,
    factor_sem, inverse_sem, first_sems, part_sems, sent_sems, tail_sems,
):
    sections = len(factor)
    rows_dev, tile, width = factor[0].shape
    rhs_count = rhs.shape[0]
    r, c = lax.axis_index("row"), lax.axis_index("col")

    loads = []
    for u in range(sections):
        pair = (
            pltpu.make_async_copy(inverse_hbm.at[u], inverse.at[u], inverse_sem.at[u]),
            pltpu.make_async_copy(factor_hbm.at[u], factor[u], factor_sem.at[u]),
        )
        for copy in pair:
            copy.start()
        loads.append(pair)

    barrier = pltpu.get_barrier_semaphore()
    for axis, me, count in (("row", r, rows), ("col", c, cols)):
        for d in range(1, count):
            pl.semaphore_signal(
                barrier, inc=1, device_id={axis: lax.rem(me + d, count)}, device_id_type=MESH
            )

    slots = [order[u] for u in range(sections)]
    roots = [lax.div(s, rows_dev) for s in slots]
    locals_ = [lax.rem(s, rows_dev) for s in slots]
    row_ids = lax.broadcasted_iota(jnp.int32, (rhs_count, width), 0)
    limit = jnp.zeros((rhs_count, width), jnp.int32)
    for k in range(rhs_count):
        limit = jnp.where(row_ids == k, live[k], limit)

    def rhs_of(local):
        picked = rhs[:, 0, :]
        for j in range(1, rows_dev):
            picked = jnp.where(local == j, rhs[:, j, :], picked)
        return picked

    for j in range(rows_dev):
        acc[j] = jnp.zeros((rhs_count, tile), jnp.float32)
    first[r] = rhs_of(locals_[0])

    pl.semaphore_wait(barrier, rows - 1 + cols - 1)

    pending = []
    copies = []
    for d in range(1, rows):
        copy = remote(
            first.at[r], first.at[r], first_sems.at[0, d], first_sems.at[1, d],
            "row", lax.rem(r + d, rows),
        )
        copy.start()
        copies.append(copy)
    pending += copies

    own = None
    for t in range(sections):
        for copy in copies:
            copy.wait_recv()
        if t == 0:
            remaining = jnp.concatenate([first[s] for s in range(rows)], axis=1)
            kept = first[r]
        else:
            remaining = own
            for d in range(1, rows):
                remaining = remaining + part_in[t, d]
            kept = remaining[:, :width]
            for s in range(1, rows):
                kept = jnp.where(r == s, remaining[:, s * width:(s + 1) * width], kept)
        high = remaining.astype(jnp.bfloat16)
        rest = remaining - high.astype(jnp.float32)
        middle = rest.astype(jnp.bfloat16)
        low = (rest - middle.astype(jnp.float32)).astype(jnp.bfloat16)
        loads[t][0].wait()
        parts = lax.dot_general(
            jnp.concatenate([high, middle, low], axis=0), inverse[t], NT,
            preferred_element_type=jnp.float32,
        )
        solved = (
            parts[2 * rhs_count:] + parts[rhs_count:2 * rhs_count]
        ) + parts[:rhs_count]
        is_live = limit > t
        sent_all[t][c] = jnp.where(is_live, solved, 0.0).astype(jnp.bfloat16)
        sends = []
        for d in range(1, cols):
            copy = remote(
                sent_all[t].at[c], sent_all[t].at[c], sent_sems.at[0, t, d],
                sent_sems.at[1, t, d], "col", lax.rem(c + d, cols),
            )
            copy.start()
            sends.append(copy)
        pending += sends
        stored[t] = jnp.where(is_live, solved, kept)
        loads[t][1].wait()
        for copy in sends:
            copy.wait_recv()
        sent = sent_all[t][roots[t]]
        if t + 1 < sections:
            local = locals_[t + 1]
            update = acc[local] + lax.dot_general(
                sent, factor[t][local], NT, preferred_element_type=jnp.float32
            )
            mine = rhs_of(local)
            own = jnp.concatenate(
                [jnp.where(r == s, mine, 0.0) for s in range(rows)], axis=1
            ) - update
            part_out[t + 1] = own
            copies = []
            for d in range(1, rows):
                copy = remote(
                    part_out.at[t + 1], part_in.at[t + 1, d], part_sems.at[0, t + 1, d],
                    part_sems.at[1, t + 1, d], "row", lax.rem(r + d, rows),
                )
                copy.start()
                copies.append(copy)
            pending += copies
            for j in range(rows_dev):
                acc[j] += lax.dot_general(
                    sent, factor[t][j], NT, preferred_element_type=jnp.float32
                )
        else:
            for j in range(rows_dev):
                total = acc[j] + lax.dot_general(
                    sent, factor[t][j], NT, preferred_element_type=jnp.float32
                )
                for s in range(rows):
                    tail_out[s, j] = total[:, s * width:(s + 1) * width]

    tails = []
    for d in range(1, rows):
        peer = lax.rem(r + d, rows)
        copy = remote(
            tail_out.at[peer], tail_in.at[d], tail_sems.at[0, d], tail_sems.at[1, d], "row", peer
        )
        copy.start()
        tails.append(copy)
    pending += tails
    for copy in tails:
        copy.wait_recv()
    for j in range(rows_dev):
        total = tail_out[r, j]
        for d in range(1, rows):
            total = total + tail_in[d, j]
        value = rhs[:, j, :] - total
        for t in range(sections):
            value = jnp.where(slots[t] == c * rows_dev + j, stored[t], value)
        out[:, j, :] = value
    for copy in pending:
        copy.wait_send()


def per_device(rows, cols, factor, diag_inverse, right_side, tile_order, live_segments):
    sections, width, tile = diag_inverse.shape
    rhs_count, rows_dev, _ = right_side.shape
    panel = jnp.transpose(factor, (1, 0, 2)).reshape(sections, rows_dev, tile, width)
    vmem = pl.BlockSpec(memory_space=pltpu.VMEM)
    smem = pl.BlockSpec(memory_space=pltpu.SMEM)
    hbm = pl.BlockSpec(memory_space=pl.ANY)
    f32, bf16 = jnp.float32, jnp.bfloat16
    return pl.pallas_call(
        functools.partial(kernel, rows, cols),
        out_shape=jax.ShapeDtypeStruct(right_side.shape, f32),
        in_specs=[hbm, hbm, vmem, smem, smem],
        out_specs=vmem,
        scratch_shapes=[
            [pltpu.VMEM((rows_dev, tile, width), bf16)] * sections,
            pltpu.VMEM((sections, width, tile), bf16),
            pltpu.VMEM((rows, rhs_count, width), f32),
            pltpu.VMEM((sections, rhs_count, tile), f32),
            pltpu.VMEM((sections, rows, rhs_count, tile), f32),
            [pltpu.VMEM((cols, rhs_count, width), bf16)] * sections,
            pltpu.VMEM((sections, rhs_count, width), f32),
            pltpu.VMEM((rows_dev, rhs_count, tile), f32),
            pltpu.VMEM((rows, rows_dev, rhs_count, width), f32),
            pltpu.VMEM((rows, rows_dev, rhs_count, width), f32),
            pltpu.SemaphoreType.DMA((sections,)),
            pltpu.SemaphoreType.DMA((sections,)),
            pltpu.SemaphoreType.DMA((2, rows)),
            pltpu.SemaphoreType.DMA((2, sections, rows)),
            pltpu.SemaphoreType.DMA((2, sections, cols)),
            pltpu.SemaphoreType.DMA((2, rows)),
        ],
        compiler_params=pltpu.CompilerParams(
            collective_id=0, has_side_effects=True, vmem_limit_bytes=48 * 2**20
        ),
    )(panel, diag_inverse, right_side, tile_order, live_segments)


def solution(mesh):
    return jax.shard_map(
        functools.partial(per_device, mesh.shape["row"], mesh.shape["col"]),
        mesh=mesh,
        in_specs=(P("col", None, "row"), P(None, "row", None), P(None, "col", "row"), P(), P()),
        out_specs=P(None, "col", "row"),
        check_vma=False,
    )
```

```python
import functools
import jax
import jax.numpy as jnp
from jax import lax
from jax.experimental import pallas as pl
from jax.experimental.pallas import tpu as pltpu
from jax.sharding import PartitionSpec as P

MESH = pl.DeviceIdType.MESH
SPARE = 128
NT = (((1,), (1,)), ((), ()))


def encode(value, spare):
    peak = jnp.max(jnp.abs(value), axis=1, keepdims=True)
    power = jnp.ceil(jnp.log2(jnp.maximum(peak, 1e-30)))
    coded = jnp.floor(value * jnp.exp2(14.0 - power) + 0.5)
    powers = jnp.broadcast_to(power, (value.shape[0], spare))
    both = jnp.concatenate([coded, powers], axis=1)
    return both.astype(jnp.int32).astype(jnp.int16)


def decode(coded, count):
    numbers = coded.astype(jnp.int32).astype(jnp.float32)
    scale = jnp.exp2(numbers[:, count:count + 1] - 14.0)
    return numbers[:, :count] * scale


def remote(src, dst, send_sem, recv_sem, axis, peer):
    return pltpu.make_async_remote_copy(
        src_ref=src, dst_ref=dst, send_sem=send_sem, recv_sem=recv_sem,
        device_id={axis: peer}, device_id_type=MESH,
    )


def kernel(
    rows, cols, factor_hbm, inverse_hbm, rhs_hbm, order_hbm, live_hbm, out,
    factor, inverse, first, part_out, part_in, sent_all, stored, acc, tail_own, tail_out, tail_in,
    rhs, order, live,
    factor_sem, inverse_sem, first_sems, part_sems, sent_sems, tail_sems, small_sem,
):
    sections = len(factor)
    rows_dev, tile, width = factor[0].shape
    rhs_count = rhs.shape[0]
    r, c = lax.axis_index("row"), lax.axis_index("col")

    small = (
        pltpu.make_async_copy(rhs_hbm, rhs, small_sem.at[0]),
        pltpu.make_async_copy(order_hbm, order, small_sem.at[1]),
        pltpu.make_async_copy(live_hbm, live, small_sem.at[2]),
    )
    for copy in small:
        copy.start()
    loads = []
    for u in range(sections):
        pair = (
            pltpu.make_async_copy(inverse_hbm.at[u], inverse.at[u], inverse_sem.at[u]),
            pltpu.make_async_copy(factor_hbm.at[u], factor[u], factor_sem.at[u]),
        )
        for copy in pair:
            copy.start()
        loads.append(pair)

    barrier = pltpu.get_barrier_semaphore()
    for axis, me, count in (("row", r, rows), ("col", c, cols)):
        for d in range(1, count):
            pl.semaphore_signal(
                barrier, inc=1, device_id={axis: lax.rem(me + d, count)}, device_id_type=MESH
            )

    for copy in small:
        copy.wait()
    slots = [order[u] for u in range(sections)]
    roots = [lax.div(s, rows_dev) for s in slots]
    locals_ = [lax.rem(s, rows_dev) for s in slots]
    row_ids = lax.broadcasted_iota(jnp.int32, (rhs_count, width), 0)
    limit = jnp.zeros((rhs_count, width), jnp.int32)
    for k in range(rhs_count):
        limit = jnp.where(row_ids == k, live[k], limit)

    def rhs_of(local):
        picked = rhs[:, 0, :]
        for j in range(1, rows_dev):
            picked = jnp.where(local == j, rhs[:, j, :], picked)
        return picked

    for j in range(rows_dev):
        acc[j] = jnp.zeros((rhs_count, tile), jnp.float32)
    first[r] = rhs_of(locals_[0])

    pl.semaphore_wait(barrier, rows - 1 + cols - 1)

    pending = []
    copies = []
    for d in range(1, rows):
        copy = remote(
            first.at[r], first.at[r], first_sems.at[0, d], first_sems.at[1, d],
            "row", lax.rem(r + d, rows),
        )
        copy.start()
        copies.append(copy)
    pending += copies

    own = None
    for t in range(sections):
        for copy in copies:
            copy.wait_recv()
        if t == 0:
            remaining = jnp.concatenate([first[s] for s in range(rows)], axis=1)
            kept = first[r]
        else:
            remaining = own
            for d in range(1, rows):
                remaining = remaining + decode(part_in[t, d], tile)
            kept = remaining[:, :width]
            for s in range(1, rows):
                kept = jnp.where(r == s, remaining[:, s * width:(s + 1) * width], kept)
        high = remaining.astype(jnp.bfloat16)
        rest = remaining - high.astype(jnp.float32)
        middle = rest.astype(jnp.bfloat16)
        low = (rest - middle.astype(jnp.float32)).astype(jnp.bfloat16)
        loads[t][0].wait()
        parts = lax.dot_general(
            jnp.concatenate([high, middle, low], axis=0), inverse[t], NT,
            preferred_element_type=jnp.float32,
        )
        solved = (
            parts[2 * rhs_count:] + parts[rhs_count:2 * rhs_count]
        ) + parts[:rhs_count]
        is_live = limit > t
        sent_all[t][c] = jnp.where(is_live, solved, 0.0).astype(jnp.bfloat16)
        sends = []
        for d in range(1, cols):
            copy = remote(
                sent_all[t].at[c], sent_all[t].at[c], sent_sems.at[0, t, d],
                sent_sems.at[1, t, d], "col", lax.rem(c + d, cols),
            )
            copy.start()
            sends.append(copy)
        pending += sends
        stored[t] = jnp.where(is_live, solved, kept)
        loads[t][1].wait()
        for copy in sends:
            copy.wait_recv()
        sent = sent_all[t][roots[t]]
        if t + 1 < sections:
            local = locals_[t + 1]
            update = acc[local] + lax.dot_general(
                sent, factor[t][local], NT, preferred_element_type=jnp.float32
            )
            mine = rhs_of(local)
            own = jnp.concatenate(
                [jnp.where(r == s, mine, 0.0) for s in range(rows)], axis=1
            ) - update
            part_out[t + 1] = encode(own, SPARE)
            copies = []
            for d in range(1, rows):
                copy = remote(
                    part_out.at[t + 1], part_in.at[t + 1, d], part_sems.at[0, t + 1, d],
                    part_sems.at[1, t + 1, d], "row", lax.rem(r + d, rows),
                )
                copy.start()
                copies.append(copy)
            pending += copies
            for j in range(rows_dev):
                acc[j] += lax.dot_general(
                    sent, factor[t][j], NT, preferred_element_type=jnp.float32
                )
        else:
            for j in range(rows_dev):
                total = acc[j] + lax.dot_general(
                    sent, factor[t][j], NT, preferred_element_type=jnp.float32
                )
                mine = total[:, :width]
                for s in range(1, rows):
                    mine = jnp.where(r == s, total[:, s * width:(s + 1) * width], mine)
                tail_own[j] = mine
                for s in range(rows):
                    tail_out[s, j] = encode(total[:, s * width:(s + 1) * width], SPARE)

    tails = []
    for d in range(1, rows):
        peer = lax.rem(r + d, rows)
        copy = remote(
            tail_out.at[peer], tail_in.at[d], tail_sems.at[0, d], tail_sems.at[1, d], "row", peer
        )
        copy.start()
        tails.append(copy)
    pending += tails
    for copy in tails:
        copy.wait_recv()
    for j in range(rows_dev):
        total = tail_own[j]
        for d in range(1, rows):
            total = total + decode(tail_in[d, j], width)
        value = rhs[:, j, :] - total
        for t in range(sections):
            value = jnp.where(slots[t] == c * rows_dev + j, stored[t], value)
        out[:, j, :] = value
    for copy in pending:
        copy.wait_send()


def per_device(rows, cols, factor, diag_inverse, right_side, tile_order, live_segments):
    sections, width, tile = diag_inverse.shape
    rhs_count, rows_dev, _ = right_side.shape
    panel = jnp.transpose(factor, (1, 0, 2)).reshape(sections, rows_dev, tile, width)
    vmem = pl.BlockSpec(memory_space=pltpu.VMEM)
    hbm = pl.BlockSpec(memory_space=pl.ANY)
    f32, bf16, i16 = jnp.float32, jnp.bfloat16, jnp.int16
    return pl.pallas_call(
        functools.partial(kernel, rows, cols),
        out_shape=jax.ShapeDtypeStruct(right_side.shape, f32),
        in_specs=[hbm] * 5,
        out_specs=vmem,
        scratch_shapes=[
            [pltpu.VMEM((rows_dev, tile, width), bf16)] * sections,
            pltpu.VMEM((sections, width, tile), bf16),
            pltpu.VMEM((rows, rhs_count, width), f32),
            pltpu.VMEM((sections, rhs_count, tile + SPARE), i16),
            pltpu.VMEM((sections, rows, rhs_count, tile + SPARE), i16),
            [pltpu.VMEM((cols, rhs_count, width), bf16)] * sections,
            pltpu.VMEM((sections, rhs_count, width), f32),
            pltpu.VMEM((rows_dev, rhs_count, tile), f32),
            pltpu.VMEM((rows_dev, rhs_count, width), f32),
            pltpu.VMEM((rows, rows_dev, rhs_count, width + SPARE), i16),
            pltpu.VMEM((rows, rows_dev, rhs_count, width + SPARE), i16),
            pltpu.VMEM(right_side.shape, f32),
            pltpu.SMEM(tile_order.shape, jnp.int32),
            pltpu.SMEM(live_segments.shape, jnp.int32),
            pltpu.SemaphoreType.DMA((sections,)),
            pltpu.SemaphoreType.DMA((sections,)),
            pltpu.SemaphoreType.DMA((2, rows)),
            pltpu.SemaphoreType.DMA((2, sections, rows)),
            pltpu.SemaphoreType.DMA((2, sections, cols)),
            pltpu.SemaphoreType.DMA((2, rows)),
            pltpu.SemaphoreType.DMA((3,)),
        ],
        compiler_params=pltpu.CompilerParams(
            collective_id=0, has_side_effects=True, vmem_limit_bytes=67043328
        ),
    )(panel, diag_inverse, right_side, tile_order, live_segments)


def solution(mesh):
    return jax.shard_map(
        functools.partial(per_device, mesh.shape["row"], mesh.shape["col"]),
        mesh=mesh,
        in_specs=(P("col", None, "row"), P(None, "row", None), P(None, "col", "row"), P(), P()),
        out_specs=P(None, "col", "row"),
        check_vma=False,
    )
```
